32 devices in a mesh: expert: 4 (over x, core), rows: 8 (over z, y).
Axes of the slice: x: 2, y: 2, z: 4, core: 2. Of those that a mesh axis runs over, the one named last changes fastest.
Arguments:
- step: int32 [], replicated, may hold values from 2 to 8
- gradient: bfloat16 [4, 4096, 14336], P('expert', 'rows'), may hold values from -8 to 8
- weight: bfloat16 [4, 4096, 14336], P('expert', 'rows'), may hold values from -0.119628906 to 0.119628906
- row_state: float32 [4, 4096], P('expert', 'rows'), may hold values from 0.3 to 3
- col_state: float32 [4, 14336], P('expert', 'rows'), may hold values from 0.3 to 3
- prev_msq: float32 [4, 8], P('expert', 'rows'), may hold values from 2 to 500
Outputs:
- new_weight: bfloat16 [4, 4096, 14336], P('expert', 'rows')
- new_row_state: float32 [4, 4096], P('expert', 'rows')
- new_col_state: float32 [4, 14336], P('expert', 'rows')
- new_msq: float32 [4, 8], P('expert', 'rows')
The draws below stay inside these ranges and needn't reach their ends.
All inputs are finite; a program needn't handle non-finite values.
Results may differ from the reference program's by a relative error of at most 0.001.
Values sent between devices are 32-bit elements; how exact they have to be, the bound alone decides.
A program may use at most 128 MiB of HBM per device.

```python
import math
import jax
import jax.numpy as jnp
from jax import lax

D = 4096
FF = 14336
EXPERTS = 4
N_ROWS = 8


def draw_gradient(key, part):
    row_blocks = 2 * N_ROWS
    block_rows = D // row_blocks
    col_blocks = FF // 8
    level_key = jax.random.fold_in(key, 11)
    noise_key = jax.random.fold_in(key, 23)
    spread = 1.0
    noise = jax.random.normal(noise_key, (EXPERTS, row_blocks, block_rows, col_blocks, 8), jnp.float32)
    levels = jnp.exp(jax.random.uniform(level_key, (EXPERTS, row_blocks, 1, col_blocks, 1), jnp.float32, -spread, spread))
    values = jnp.clip(noise * levels, -8.0, 8.0)
    return values.reshape(EXPERTS, D, FF).astype(jnp.bfloat16)


def block_scale(rng, extent, pieces, smallest, high):
    factor_of, own = 1.0, jax.random.fold_in(rng, 6)
    for dim, parts in pieces:
        draws = jnp.exp(jax.random.uniform(jax.random.fold_in(own, dim), (parts,), jnp.float32, smallest / len(pieces), high / len(pieces)))
        factor_of = factor_of * jnp.repeat(draws, extent[dim] // parts).reshape([-1 if axis == dim else 1 for axis in range(len(extent))])
    return factor_of


def bell_draw(stream_key, dims, width, reach, shards=(), dtype=jnp.bfloat16):
    result = jax.random.normal(stream_key, dims, jnp.float32) * width
    if len(shards) > 0:
        result = block_scale(stream_key, dims, shards, -0.22, 0.18) * result
    return jnp.clip(result, min=-reach, max=reach).astype(dtype)


def setup_inputs(seed: int = 0) -> dict:
    key_of = jax.random.split(jax.random.key(seed), 7)
    step = jax.random.randint(key_of[0], (), 2, 9).astype(jnp.int32)
    gradient = draw_gradient(jax.random.fold_in(key_of[6], 71), 0)
    weight = bell_draw(key_of[2], (EXPERTS, D, FF), 0.02, 0.119628906, ((0, 4), (1, 8)))
    row_state = jnp.clip(jnp.exp(math.log(3.0) - 2.3025851 * jax.random.uniform(key_of[3], (EXPERTS, D), jnp.float32) ** block_scale(key_of[3], (EXPERTS, D), ((0, 4), (1, 8)), -0.2, 0.2)), 0.3, 3.0)
    col_state = jnp.clip(jnp.exp(math.log(3.0) - 2.3025851 * jax.random.uniform(key_of[4], (EXPERTS, FF), jnp.float32) ** block_scale(key_of[4], (EXPERTS, FF), ((0, 4), (1, 8)), -0.2, 0.2)), 0.3, 3.0)
    prev_msq = jnp.clip(jnp.exp(math.log(500.0) - 5.521461 * jax.random.uniform(key_of[5], (EXPERTS, N_ROWS), jnp.float32) ** block_scale(key_of[5], (EXPERTS, N_ROWS), ((0, 4), (1, 8)), -0.2, 0.2)), 2.0, 500.0)
    return dict(step=step, gradient=gradient, weight=weight, row_state=row_state, col_state=col_state, prev_msq=prev_msq)


def one_expert(inputs):
    gradient, weight, row_state, col_state, beta, clip = inputs
    grad = gradient.astype(jnp.float32)
    squares = grad * grad + 1e-30
    new_row = beta * row_state + (1.0 - beta) * lax.optimization_barrier(jnp.mean(squares, axis=1))
    new_col = beta * col_state + (1.0 - beta) * lax.optimization_barrier(jnp.sum(squares, axis=0)) / D
    row_mean = jnp.mean(new_row)
    scaled = new_row[:, None] * new_col[None, :] / row_mean
    update = grad / jnp.sqrt(scaled) / clip
    new_weight = (weight.astype(jnp.float32) - 0.01 * update).astype(jnp.bfloat16)
    blocks = (update * update).reshape(N_ROWS, D // N_ROWS, FF)
    new_msq = lax.optimization_barrier(jnp.mean(blocks, axis=(1, 2)))
    return (new_weight, new_row, new_col, new_msq)

def reference(step, gradient, weight, row_state, col_state, prev_msq):
    beta = 1.0 - step.astype(jnp.float32) ** (-0.8)
    clip = jnp.sqrt(jnp.mean(prev_msq))
    count = gradient.shape[0]
    betas = jnp.full((count,), beta, jnp.float32)
    clips = jnp.full((count,), clip, jnp.float32)
    new_weight, new_row, new_col, new_msq = lax.map(one_expert, (gradient, weight, row_state, col_state, betas, clips))
    return (new_weight, new_row, new_col, new_msq)
```

```python
import functools

import jax
import jax.numpy as jnp
from jax import lax
from jax.experimental import pallas as pl
from jax.experimental.pallas import tpu as pltpu
from jax.sharding import PartitionSpec as P

MESH = pl.DeviceIdType.MESH
RATE = 0.01
TINY = 1e-30
LANES = 128
ROWS = 16


def lane_sum(x):
    total = x[:, :LANES]
    for k in range(1, x.shape[1] // LANES):
        total = total + x[:, k * LANES : (k + 1) * LANES]
    return total


def statistics_kernel(
    n, experts, step_ref, prev_ref, row_ref, col_ref, g_hbm, w_hbm,
    g_out, w_out, scale_out, factor_out, new_row_out, new_col_out,
    acc, part, parts_in, message, messages_in, clip_out, clips_in,
    g_sem, w_sem, clip_send, clip_recv, part_send, part_recv, gather_send, gather_recv,
):
    me = lax.axis_index("rows")
    mine = lax.axis_index("expert")
    rows, columns = g_out.shape
    width = columns // n

    def column_slice(c):
        return pl.ds(pl.multiple_of(c * width, LANES), width)

    def chunk_of(s):
        return lax.rem(me + (2 * (s % 2) - 1) * ((n - s) // 2) + n, n)

    def g_copy(s):
        cols = column_slice(chunk_of(s))
        return pltpu.make_async_copy(g_hbm.at[:, cols], g_out.at[:, cols], g_sem.at[s])

    def w_copy(s):
        cols = column_slice(s)
        return pltpu.make_async_copy(w_hbm.at[:, cols], w_out.at[:, cols], w_sem.at[s])

    def clip_copy(k):
        peer = lax.rem(mine + k, experts)
        return pltpu.make_async_remote_copy(
            src_ref=clip_out, dst_ref=clips_in.at[k - 1], send_sem=clip_send.at[k - 1],
            recv_sem=clip_recv.at[k - 1], device_id={"expert": peer}, device_id_type=MESH,
        )

    def part_copy(s):
        c = chunk_of(s)
        return pltpu.make_async_remote_copy(
            src_ref=part.at[s], dst_ref=parts_in.at[s], send_sem=part_send.at[s],
            recv_sem=part_recv.at[s], device_id={"rows": c}, device_id_type=MESH,
        )

    def gather_copy(k):
        peer = lax.rem(me + k, n)
        return pltpu.make_async_remote_copy(
            src_ref=message, dst_ref=messages_in.at[k - 1], send_sem=gather_send.at[k - 1],
            recv_sem=gather_recv.at[k - 1], device_id={"rows": peer}, device_id_type=MESH,
        )

    for s in range(n):
        g_copy(s).start()

    barrier = pltpu.get_barrier_semaphore()
    for k in range(1, n):
        pl.semaphore_signal(barrier, inc=1, device_id={"rows": lax.rem(me + k, n)}, device_id_type=MESH)
    for k in range(1, experts):
        pl.semaphore_signal(barrier, inc=1, device_id={"expert": lax.rem(mine + k, experts)}, device_id_type=MESH)

    acc[...] = jnp.zeros_like(acc)
    clip_out[...] = jnp.full((1, LANES), prev_ref[0], jnp.float32)
    beta = 1.0 - jnp.exp(-0.8 * jnp.log(jnp.full((1, LANES), step_ref[0], jnp.int32).astype(jnp.float32)))

    def chunk(s):
        cols = column_slice(chunk_of(s))
        g_copy(s).wait()

        def body(i, carry):
            at = pl.ds(pl.multiple_of(i * ROWS, ROWS), ROWS)
            x = g_out[at, cols].astype(jnp.float32)
            squares = x * x
            acc[at, :] += lane_sum(squares)
            return carry + (squares[: ROWS // 2] + squares[ROWS // 2 :])

        col = lax.fori_loop(0, rows // ROWS, body, jnp.zeros((ROWS // 2, width), jnp.float32))
        part[s] = jnp.sum(col, axis=0, keepdims=True)

    half = n // 2

    @pl.loop(0, half)
    def _(s):
        chunk(s)

    pl.semaphore_wait(barrier, n - 1 + experts - 1)
    for k in range(1, experts):
        clip_copy(k).start()
    for s in range(half):
        part_copy(s).start()

    @pl.loop(half, n - 1)
    def _(s):
        w_copy(s - half).start()
        chunk(s)
        part_copy(s).start()

    for s in range(n - 1 - half, n):
        w_copy(s).start()
    chunk(n - 1)

    share = lane_sum(row_ref[...]) * beta
    share = share + (1.0 - beta) * (jnp.sum(acc[...], axis=0, keepdims=True) * (1.0 / columns) + TINY * (rows / LANES))
    clips = clip_out[...]
    for k in range(1, experts):
        clip_copy(k).wait()
        clips = clips + clips_in[k - 1]
    total = part[n - 1]
    for s in range(n - 1):
        part_copy(s).wait()
        total = total + parts_in[s]
    beta_cols = jnp.concatenate([beta] * (width // LANES), axis=1)
    new_col = beta_cols * col_ref[...] + (1.0 - beta_cols) * (total * (1.0 / (rows * n)) + TINY)
    message[:, :width] = new_col
    message[:, width : width + LANES] = share
    message[:, width + LANES :] = clips
    for k in range(1, n):
        gather_copy(k).start()

    new_col_out[...] = new_col
    factor_out[:, column_slice(me)] = lax.rsqrt(new_col)
    sums = jnp.sum(jnp.transpose(acc[...]), axis=0, keepdims=True)
    beta_rows = jnp.concatenate([beta] * (rows // LANES), axis=1)
    new_row = beta_rows * row_ref[...] + (1.0 - beta_rows) * (sums * (1.0 / columns) + TINY)
    new_row_out[...] = new_row
    for s in range(n):
        w_copy(s).wait()

    for k in range(1, n):
        gather_copy(k).wait()
        source = lax.rem(me - k + n, n)
        factor_out[:, column_slice(source)] = lax.rsqrt(messages_in[k - 1, :, :width])
        share = share + messages_in[k - 1, :, width : width + LANES]
        clips = clips + messages_in[k - 1, :, width + LANES :]
    row_mean = jnp.sum(share, axis=1, keepdims=True) * (1.0 / (rows * n))
    clip = jnp.sqrt(clips[:, :1] * (1.0 / (n * experts)))
    scale = lax.rsqrt(new_row / row_mean) * (RATE / clip)
    scale_out[...] = jnp.transpose(jnp.broadcast_to(scale, (LANES, rows)))


def update_kernel(
    block, g_ref, w_ref, scale_ref, factor_ref, row_ref, col_ref,
    new_w_hbm, new_row_out, new_col_out, msq_out, stage, sem,
):
    rows, columns = g_ref.shape
    blocks = columns // block

    def out_copy(b):
        cols = pl.ds(pl.multiple_of(b * block, LANES), block)
        return pltpu.make_async_copy(stage.at[b % 2], new_w_hbm.at[:, cols], sem.at[b % 2])

    new_row_out[...] = row_ref[...]
    new_col_out[...] = col_ref[...]

    def do_block(b, total):
        cols = pl.ds(pl.multiple_of(b * block, LANES), block)
        slot = b % 2

        @pl.when(b >= 2)
        def _():
            out_copy(b - 2).wait()

        factor = jnp.broadcast_to(factor_ref[:, cols], (ROWS, block))

        def body(i, total):
            at = pl.ds(pl.multiple_of(i * ROWS, ROWS), ROWS)
            scale = jnp.concatenate([scale_ref[at, :]] * (block // LANES), axis=1)
            move = g_ref[at, cols].astype(jnp.float32) * factor * scale
            stage[slot, at, :] = (w_ref[at, cols].astype(jnp.float32) - move).astype(jnp.bfloat16)
            return total + lane_sum(move * move)

        total = lax.fori_loop(0, rows // ROWS, body, total)
        out_copy(b).start()
        return total

    total = lax.fori_loop(0, blocks, do_block, jnp.zeros((ROWS, LANES), jnp.float32))
    for b in range(max(blocks - 2, 0), blocks):
        out_copy(b).wait()
    msq = jnp.sum(jnp.sum(total, axis=0, keepdims=True), axis=1, keepdims=True)
    msq_out[...] = msq * (1.0 / (RATE * RATE * rows * columns))


def block_width(columns):
    tiles = columns // LANES
    for d in (8, 7, 4, 2, 1):
        if tiles % d == 0:
            return d * LANES


def shards(step, gradient, weight, row_state, col_state, prev_msq):
    _, rows, columns = gradient.shape
    n = lax.axis_size("rows")
    experts = lax.axis_size("expert")
    width = columns // n
    f32, bf16 = jnp.float32, gradient.dtype
    vmem = pl.BlockSpec(memory_space=pltpu.VMEM)
    smem = pl.BlockSpec(memory_space=pltpu.SMEM)
    anywhere = pl.BlockSpec(memory_space=pl.ANY)
    dma = pltpu.SemaphoreType.DMA
    big = rows * columns * 2
    g, w, scale, factor, new_row, new_col = pl.pallas_call(
        functools.partial(statistics_kernel, n, experts),
        out_shape=[
            pltpu.VMEM((rows, columns), bf16),
            pltpu.VMEM((rows, columns), bf16),
            pltpu.VMEM((rows, LANES), f32),
            pltpu.VMEM((1, columns), f32),
            pltpu.VMEM((1, rows), f32),
            pltpu.VMEM((1, width), f32),
        ],
        in_specs=[smem, smem, vmem, vmem, anywhere, anywhere],
        out_specs=[vmem] * 6,
        scratch_shapes=[
            pltpu.VMEM((rows, LANES), f32),
            pltpu.VMEM((n, 1, width), f32),
            pltpu.VMEM((n - 1, 1, width), f32),
            pltpu.VMEM((1, width + 2 * LANES), f32),
            pltpu.VMEM((n - 1, 1, width + 2 * LANES), f32),
            pltpu.VMEM((1, LANES), f32),
            pltpu.VMEM((experts - 1, 1, LANES), f32),
            dma((n,)), dma((n,)), dma((experts - 1,)), dma((experts - 1,)),
            dma((n - 1,)), dma((n - 1,)), dma((n - 1,)), dma((n - 1,)),
        ],
        compiler_params=pltpu.CompilerParams(
            collective_id=0, has_side_effects=True, vmem_limit_bytes=8 * 2**20
        ),
        name="statistics",
    )(
        step.reshape(1), prev_msq.reshape(1), row_state, col_state,
        gradient.reshape(rows, columns), weight.reshape(rows, columns),
    )
    block = block_width(columns)
    g, w, scale, factor, new_row, new_col = (
        pltpu.with_memory_space_constraint(x, pltpu.VMEM) for x in (g, w, scale, factor, new_row, new_col)
    )
    new_weight, new_row, new_col, msq = pl.pallas_call(
        functools.partial(update_kernel, block),
        out_shape=[
            jax.ShapeDtypeStruct((rows, columns), bf16),
            jax.ShapeDtypeStruct((1, rows), f32),
            jax.ShapeDtypeStruct((1, width), f32),
            jax.ShapeDtypeStruct((1, 1), f32),
        ],
        in_specs=[vmem] * 6,
        out_specs=[anywhere, vmem, vmem, vmem],
        scratch_shapes=[pltpu.VMEM((2, rows, block), bf16), dma((2,))],
        compiler_params=pltpu.CompilerParams(vmem_limit_bytes=8 * 2**20),
        name="update",
    )(g, w, scale, factor, new_row, new_col)
    return (new_weight.reshape(1, rows, columns), new_row, new_col, msq)


def solution(mesh):
    split = P("expert", "rows")
    whole = P("expert", "rows", None)
    return jax.shard_map(
        shards,
        mesh=mesh,
        in_specs=(P(), whole, whole, split, split, split),
        out_specs=(whole, split, split, split),
        check_vma=False,
    )
```

```python
import functools

import jax
import jax.numpy as jnp
from jax import lax
from jax.experimental import pallas as pl
from jax.experimental.pallas import tpu as pltpu
from jax.sharding import PartitionSpec as P

MESH = pl.DeviceIdType.MESH
RATE = 0.01
TINY = 1e-30
LANES = 128
ROWS = 16


def lane_sum(x):
    total = x[:, :LANES]
    for k in range(1, x.shape[1] // LANES):
        total = total + x[:, k * LANES : (k + 1) * LANES]
    return total


def statistics_kernel(
    n, experts, step_ref, prev_ref, row_hbm, col_hbm, g_hbm, w_hbm,
    g_out, w_out, scale_out, factor_out, new_row_out, new_col_out,
    acc, part, parts_in, message, messages_in, clip_out, clips_in,
    row_ref, col_ref, small_sem, g_sem, w_sem, clip_send, clip_recv, part_send, part_recv, gather_send, gather_recv,
):
    me = lax.axis_index("rows")
    mine = lax.axis_index("expert")
    rows, columns = g_out.shape
    width = columns // n

    def column_slice(c):
        return pl.ds(pl.multiple_of(c * width, LANES), width)

    def chunk_of(s):
        return lax.rem(me + (2 * (s % 2) - 1) * ((n - s) // 2) + n, n)

    def g_copy(s):
        cols = column_slice(chunk_of(s))
        return pltpu.make_async_copy(g_hbm.at[:, cols], g_out.at[:, cols], g_sem.at[s])

    def w_copy(s):
        cols = column_slice(s)
        return pltpu.make_async_copy(w_hbm.at[:, cols], w_out.at[:, cols], w_sem.at[s])

    def clip_copy(k):
        peer = lax.rem(mine + k, experts)
        return pltpu.make_async_remote_copy(
            src_ref=clip_out, dst_ref=clips_in.at[k - 1], send_sem=clip_send.at[k - 1],
            recv_sem=clip_recv.at[k - 1], device_id={"expert": peer}, device_id_type=MESH,
        )

    def part_copy(s):
        c = chunk_of(s)
        return pltpu.make_async_remote_copy(
            src_ref=part.at[s], dst_ref=parts_in.at[s], send_sem=part_send.at[s],
            recv_sem=part_recv.at[s], device_id={"rows": c}, device_id_type=MESH,
        )

    def gather_copy(k):
        peer = lax.rem(me + k, n)
        return pltpu.make_async_remote_copy(
            src_ref=message, dst_ref=messages_in.at[k - 1], send_sem=gather_send.at[k - 1],
            recv_sem=gather_recv.at[k - 1], device_id={"rows": peer}, device_id_type=MESH,
        )

    pairs = ((row_hbm, row_ref), (col_hbm, col_ref))
    small = [pltpu.make_async_copy(src, dst, small_sem.at[k]) for k, (src, dst) in enumerate(pairs)]
    for copy in small:
        copy.start()
    for s in range(n):
        g_copy(s).start()

    barrier = pltpu.get_barrier_semaphore()
    for k in range(1, n):
        pl.semaphore_signal(barrier, inc=1, device_id={"rows": lax.rem(me + k, n)}, device_id_type=MESH)
    for k in range(1, experts):
        pl.semaphore_signal(barrier, inc=1, device_id={"expert": lax.rem(mine + k, experts)}, device_id_type=MESH)

    acc[...] = jnp.zeros_like(acc)
    for copy in small:
        copy.wait()
    clip_out[...] = jnp.full((1, LANES), prev_ref[0], jnp.float32)
    beta = 1.0 - jnp.exp(-0.8 * jnp.log(jnp.full((1, LANES), step_ref[0], jnp.int32).astype(jnp.float32)))

    def chunk(s):
        cols = column_slice(chunk_of(s))
        g_copy(s).wait()

        def body(i, carry):
            at = pl.ds(pl.multiple_of(i * ROWS, ROWS), ROWS)
            x = g_out[at, cols].astype(jnp.float32)
            squares = x * x
            acc[at, :] += lane_sum(squares)
            return carry + (squares[: ROWS // 2] + squares[ROWS // 2 :])

        col = lax.fori_loop(0, rows // ROWS, body, jnp.zeros((ROWS // 2, width), jnp.float32))
        part[s] = jnp.sum(col, axis=0, keepdims=True)

    half = n // 2

    @pl.loop(0, half)
    def _(s):
        chunk(s)

    pl.semaphore_wait(barrier, n - 1 + experts - 1)
    for k in range(1, experts):
        clip_copy(k).start()
    for s in range(half):
        part_copy(s).start()

    @pl.loop(half, n - 1)
    def _(s):
        w_copy(s - half).start()
        chunk(s)
        part_copy(s).start()

    for s in range(n - 1 - half, n):
        w_copy(s).start()
    chunk(n - 1)

    share = lane_sum(row_ref[...]) * beta
    share = share + (1.0 - beta) * (jnp.sum(acc[...], axis=0, keepdims=True) * (1.0 / columns) + TINY * (rows / LANES))
    clips = clip_out[...]
    for k in range(1, experts):
        clip_copy(k).wait()
        clips = clips + clips_in[k - 1]
    total = part[n - 1]
    for s in range(n - 1):
        part_copy(s).wait()
        total = total + parts_in[s]
    beta_cols = jnp.concatenate([beta] * (width // LANES), axis=1)
    new_col = beta_cols * col_ref[...] + (1.0 - beta_cols) * (total * (1.0 / (rows * n)) + TINY)
    message[:, :width] = new_col
    message[:, width : width + LANES] = share
    message[:, width + LANES :] = clips
    for k in range(1, n):
        gather_copy(k).start()

    new_col_out[...] = new_col
    factor_out[:, column_slice(me)] = lax.rsqrt(new_col)
    sums = jnp.sum(jnp.transpose(acc[...]), axis=0, keepdims=True)
    beta_rows = jnp.concatenate([beta] * (rows // LANES), axis=1)
    new_row = beta_rows * row_ref[...] + (1.0 - beta_rows) * (sums * (1.0 / columns) + TINY)
    new_row_out[...] = new_row
    for s in range(n):
        w_copy(s).wait()

    for k in range(1, n):
        gather_copy(k).wait()
        source = lax.rem(me - k + n, n)
        factor_out[:, column_slice(source)] = lax.rsqrt(messages_in[k - 1, :, :width])
        share = share + messages_in[k - 1, :, width : width + LANES]
        clips = clips + messages_in[k - 1, :, width + LANES :]
    row_mean = jnp.sum(share, axis=1, keepdims=True) * (1.0 / (rows * n))
    clip = jnp.sqrt(clips[:, :1] * (1.0 / (n * experts)))
    scale = lax.rsqrt(new_row / row_mean) * (RATE / clip)
    scale_out[...] = jnp.transpose(jnp.broadcast_to(scale, (LANES, rows)))


def update_kernel(
    block, g_ref, w_ref, scale_ref, factor_ref, row_ref, col_ref,
    new_w_hbm, new_row_out, new_col_out, msq_out, stage, sem,
):
    rows, columns = g_ref.shape
    blocks = columns // block

    def out_copy(b):
        cols = pl.ds(pl.multiple_of(b * block, LANES), block)
        return pltpu.make_async_copy(stage.at[b % 2], new_w_hbm.at[:, cols], sem.at[b % 2])

    new_row_out[...] = row_ref[...]
    new_col_out[...] = col_ref[...]

    def do_block(b, total):
        cols = pl.ds(pl.multiple_of(b * block, LANES), block)
        slot = b % 2

        @pl.when(b >= 2)
        def _():
            out_copy(b - 2).wait()

        factor = jnp.broadcast_to(factor_ref[:, cols], (ROWS, block))

        def body(i, total):
            at = pl.ds(pl.multiple_of(i * ROWS, ROWS), ROWS)
            scale = jnp.concatenate([scale_ref[at, :]] * (block // LANES), axis=1)
            move = g_ref[at, cols].astype(jnp.float32) * factor * scale
            stage[slot, at, :] = (w_ref[at, cols].astype(jnp.float32) - move).astype(jnp.bfloat16)
            return total + lane_sum(move * move)

        total = lax.fori_loop(0, rows // ROWS, body, total)
        out_copy(b).start()
        return total

    total = lax.fori_loop(0, blocks, do_block, jnp.zeros((ROWS, LANES), jnp.float32))
    for b in range(max(blocks - 2, 0), blocks):
        out_copy(b).wait()
    msq = jnp.sum(jnp.sum(total, axis=0, keepdims=True), axis=1, keepdims=True)
    msq_out[...] = msq * (1.0 / (RATE * RATE * rows * columns))


def block_width(columns):
    tiles = columns // LANES
    for d in (8, 7, 4, 2, 1):
        if tiles % d == 0:
            return d * LANES


def shards(step, gradient, weight, row_state, col_state, prev_msq):
    _, rows, columns = gradient.shape
    n = lax.axis_size("rows")
    experts = lax.axis_size("expert")
    width = columns // n
    f32, bf16 = jnp.float32, gradient.dtype
    vmem = pl.BlockSpec(memory_space=pltpu.VMEM)
    hbm = pl.BlockSpec(memory_space=pltpu.HBM)
    dma = pltpu.SemaphoreType.DMA
    big = rows * columns * 2
    g, w, scale, factor, new_row, new_col = pl.pallas_call(
        functools.partial(statistics_kernel, n, experts),
        out_shape=[
            pltpu.VMEM((rows, columns), bf16),
            pltpu.VMEM((rows, columns), bf16),
            pltpu.VMEM((rows, LANES), f32),
            pltpu.VMEM((1, columns), f32),
            pltpu.VMEM((1, rows), f32),
            pltpu.VMEM((1, width), f32),
        ],
        in_specs=[pl.BlockSpec(memory_space=pltpu.SMEM)] * 2 + [hbm] * 4,
        out_specs=[vmem] * 6,
        scratch_shapes=[
            pltpu.VMEM((rows, LANES), f32),
            pltpu.VMEM((n, 1, width), f32),
            pltpu.VMEM((n - 1, 1, width), f32),
            pltpu.VMEM((1, width + 2 * LANES), f32),
            pltpu.VMEM((n - 1, 1, width + 2 * LANES), f32),
            pltpu.VMEM((1, LANES), f32),
            pltpu.VMEM((experts - 1, 1, LANES), f32),
            pltpu.VMEM((1, rows), f32),
            pltpu.VMEM((1, width), f32),
            dma((2,)), dma((n,)), dma((n,)), dma((experts - 1,)), dma((experts - 1,)),
            dma((n - 1,)), dma((n - 1,)), dma((n - 1,)), dma((n - 1,)),
        ],
        compiler_params=pltpu.CompilerParams(
            collective_id=0, has_side_effects=True, vmem_limit_bytes=8 * 2**20
        ),
        name="statistics",
    )(
        step.reshape(1), prev_msq.reshape(1),
        *(
            pltpu.with_memory_space_constraint(x, pltpu.HBM)
            for x in (row_state, col_state, gradient.reshape(rows, columns), weight.reshape(rows, columns))
        )
    )
    block = block_width(columns)
    new_weight, new_row, new_col, msq = pl.pallas_call(
        functools.partial(update_kernel, block),
        out_shape=[
            jax.ShapeDtypeStruct((rows, columns), bf16),
            jax.ShapeDtypeStruct((1, rows), f32),
            jax.ShapeDtypeStruct((1, width), f32),
            jax.ShapeDtypeStruct((1, 1), f32),
        ],
        in_specs=[vmem] * 6,
        out_specs=[hbm, vmem, vmem, vmem],
        scratch_shapes=[pltpu.VMEM((2, rows, block), bf16), dma((2,))],
        compiler_params=pltpu.CompilerParams(vmem_limit_bytes=8 * 2**20),
        name="update",
    )(g, w, scale, factor, new_row, new_col)
    return (new_weight.reshape(1, rows, columns), new_row, new_col, msq)


def solution(mesh):
    split = P("expert", "rows")
    whole = P("expert", "rows", None)
    return jax.shard_map(
        shards,
        mesh=mesh,
        in_specs=(P(), whole, whole, split, split, split),
        out_specs=(whole, split, split, split),
        check_vma=False,
    )
```

```python
import functools

import jax
import jax.numpy as jnp
from jax import lax
from jax.experimental import pallas as pl
from jax.experimental.pallas import tpu as pltpu
from jax.sharding import PartitionSpec as P

MESH = pl.DeviceIdType.MESH
RATE = 0.01
TINY = 1e-30
LANES = 128
ROWS = 16
UNROLL = 4


def lane_sum(x):
    total = x[:, :LANES]
    for k in range(1, x.shape[1] // LANES):
        total = total + x[:, k * LANES : (k + 1) * LANES]
    return total


def statistics_kernel(
    n, experts, step_ref, prev_ref, row_hbm, col_hbm, g_hbm, w_hbm,
    g_out, w_out, scale_out, factor_out, new_row_out, new_col_out,
    acc, part, parts_in, message, messages_in, clip_out, clips_in,
    row_ref, col_ref, small_sem, g_sem, w_sem, clip_send, clip_recv, part_send, part_recv, gather_send, gather_recv,
):
    me = lax.axis_index("rows")
    mine = lax.axis_index("expert")
    rows, columns = g_out.shape
    width = columns // n

    def column_slice(c):
        return pl.ds(pl.multiple_of(c * width, LANES), width)

    def partner(k):
        peer, bit = 0, 1
        while bit < n:
            peer = peer + bit * ((me // bit + k // bit) % 2)
            bit *= 2
        return peer

    def chunk_of(s):
        return partner(n - 1 - s)

    def g_copy(s):
        cols = column_slice(chunk_of(s))
        return pltpu.make_async_copy(g_hbm.at[:, cols], g_out.at[:, cols], g_sem.at[s])

    def w_copy(s):
        cols = column_slice(s)
        return pltpu.make_async_copy(w_hbm.at[:, cols], w_out.at[:, cols], w_sem.at[s])

    def clip_copy(k):
        peer = lax.rem(mine + k, experts)
        return pltpu.make_async_remote_copy(
            src_ref=clip_out, dst_ref=clips_in.at[k - 1], send_sem=clip_send.at[k - 1],
            recv_sem=clip_recv.at[k - 1], device_id={"expert": peer}, device_id_type=MESH,
        )

    def part_copy(s):
        c = chunk_of(s)
        return pltpu.make_async_remote_copy(
            src_ref=part.at[s], dst_ref=parts_in.at[s], send_sem=part_send.at[s],
            recv_sem=part_recv.at[s], device_id={"rows": c}, device_id_type=MESH,
        )

    def gather_copy(k):
        peer = partner(k)
        return pltpu.make_async_remote_copy(
            src_ref=message, dst_ref=messages_in.at[k - 1], send_sem=gather_send.at[k - 1],
            recv_sem=gather_recv.at[k - 1], device_id={"rows": peer}, device_id_type=MESH,
        )

    pairs = ((row_hbm, row_ref), (col_hbm, col_ref))
    small = [pltpu.make_async_copy(src, dst, small_sem.at[k]) for k, (src, dst) in enumerate(pairs)]
    for copy in small:
        copy.start()
    for s in range(n):
        g_copy(s).start()

    barrier = pltpu.get_barrier_semaphore()
    for k in range(1, n):
        pl.semaphore_signal(barrier, inc=1, device_id={"rows": lax.rem(me + k, n)}, device_id_type=MESH)
    for k in range(1, experts):
        pl.semaphore_signal(barrier, inc=1, device_id={"expert": lax.rem(mine + k, experts)}, device_id_type=MESH)

    acc[...] = jnp.zeros_like(acc)
    for copy in small:
        copy.wait()
    clip_out[...] = jnp.full((1, LANES), prev_ref[0], jnp.float32)
    beta = 1.0 - jnp.exp(-0.8 * jnp.log(jnp.full((1, LANES), step_ref[0], jnp.int32).astype(jnp.float32)))

    def chunk(s):
        cols = column_slice(chunk_of(s))
        g_copy(s).wait()

        def body(i, carry):
            at = pl.ds(pl.multiple_of(i * ROWS, ROWS), ROWS)
            x = g_out[at, cols].astype(jnp.float32)
            squares = x * x
            acc[at, :] += lane_sum(squares)
            return carry + (squares[: ROWS // 2] + squares[ROWS // 2 :])

        col = lax.fori_loop(0, rows // ROWS, body, jnp.zeros((ROWS // 2, width), jnp.float32), unroll=UNROLL)
        part[s] = jnp.sum(col, axis=0, keepdims=True)

    half = n // 2

    @pl.loop(0, half)
    def _(s):
        chunk(s)

    pl.semaphore_wait(barrier, n - 1 + experts - 1)
    for k in range(1, experts):
        clip_copy(k).start()
    for s in range(half):
        part_copy(s).start()

    @pl.loop(half, n - 1)
    def _(s):
        w_copy(s - half).start(priority=1)
        chunk(s)
        part_copy(s).start()

    for s in range(n - 1 - half, n):
        w_copy(s).start(priority=1)
    chunk(n - 1)

    share = lane_sum(row_ref[...]) * beta
    share = share + (1.0 - beta) * (jnp.sum(acc[...], axis=0, keepdims=True) * (1.0 / columns) + TINY * (rows / LANES))
    clips = clip_out[...]
    for k in range(1, experts):
        clip_copy(k).wait()
        clips = clips + clips_in[k - 1]
    total = part[n - 1]
    for s in range(n - 1):
        part_copy(s).wait()
        total = total + parts_in[s]
    beta_cols = jnp.concatenate([beta] * (width // LANES), axis=1)
    new_col = beta_cols * col_ref[...] + (1.0 - beta_cols) * (total * (1.0 / (rows * n)) + TINY)
    message[:, :width] = new_col
    message[:, width : width + LANES] = share
    message[:, width + LANES :] = clips
    for k in reversed(range(1, n)):
        gather_copy(k).start()

    new_col_out[...] = new_col
    sums = jnp.sum(jnp.transpose(acc[...]), axis=0, keepdims=True)
    beta_rows = jnp.concatenate([beta] * (rows // LANES), axis=1)
    new_row = beta_rows * row_ref[...] + (1.0 - beta_rows) * (sums * (1.0 / columns) + TINY)
    new_row_out[...] = new_row
    scale_out[...] = jnp.transpose(jnp.broadcast_to(lax.rsqrt(new_row), (LANES, rows)))
    for s in range(n):
        w_copy(s).wait()

    for k in reversed(range(1, n)):
        gather_copy(k).wait()
        share = share + messages_in[k - 1, :, width : width + LANES]
        clips = clips + messages_in[k - 1, :, width + LANES :]
    row_mean = jnp.sum(share, axis=1, keepdims=True) * (1.0 / (rows * n))
    clip_square = clips[:, :1] * (1.0 / (n * experts))
    common = RATE * jnp.sqrt(row_mean) * lax.rsqrt(clip_square)
    factor_out[:, column_slice(me)] = lax.rsqrt(new_col) * common
    for k in range(1, n):
        factor_out[:, column_slice(partner(k))] = lax.rsqrt(messages_in[k - 1, :, :width]) * common


def update_kernel(
    block, g_ref, w_ref, scale_ref, factor_ref, row_ref, col_ref,
    new_w_hbm, new_row_out, new_col_out, msq_out, stage, sem,
):
    rows, columns = g_ref.shape
    blocks = columns // block

    def out_copy(b):
        cols = pl.ds(pl.multiple_of(b * block, LANES), block)
        return pltpu.make_async_copy(stage.at[b % 2], new_w_hbm.at[:, cols], sem.at[b % 2])

    new_row_out[...] = row_ref[...]
    new_col_out[...] = col_ref[...]

    def do_block(b, total):
        cols = pl.ds(pl.multiple_of(b * block, LANES), block)
        slot = b % 2

        @pl.when(b >= 2)
        def _():
            out_copy(b - 2).wait()

        factor = jnp.broadcast_to(factor_ref[:, cols], (ROWS, block))

        def body(i, total):
            at = pl.ds(pl.multiple_of(i * ROWS, ROWS), ROWS)
            scale = jnp.concatenate([scale_ref[at, :]] * (block // LANES), axis=1)
            move = g_ref[at, cols].astype(jnp.float32) * factor * scale
            stage[slot, at, :] = (w_ref[at, cols].astype(jnp.float32) - move).astype(jnp.bfloat16)
            return total + lane_sum(move * move)

        total = lax.fori_loop(0, rows // ROWS, body, total, unroll=UNROLL)
        out_copy(b).start()
        return total

    total = lax.fori_loop(0, blocks, do_block, jnp.zeros((ROWS, LANES), jnp.float32))
    for b in range(max(blocks - 2, 0), blocks):
        out_copy(b).wait()
    msq = jnp.sum(jnp.sum(total, axis=0, keepdims=True), axis=1, keepdims=True)
    msq_out[...] = msq * (1.0 / (RATE * RATE * rows * columns))


def block_width(columns):
    tiles = columns // LANES
    for d in (8, 7, 4, 2, 1):
        if tiles % d == 0:
            return d * LANES


def shards(step, gradient, weight, row_state, col_state, prev_msq):
    _, rows, columns = gradient.shape
    n = lax.axis_size("rows")
    experts = lax.axis_size("expert")
    width = columns // n
    f32, bf16 = jnp.float32, gradient.dtype
    vmem = pl.BlockSpec(memory_space=pltpu.VMEM)
    hbm = pl.BlockSpec(memory_space=pltpu.HBM)
    dma = pltpu.SemaphoreType.DMA
    big = rows * columns * 2
    g, w, scale, factor, new_row, new_col = pl.pallas_call(
        functools.partial(statistics_kernel, n, experts),
        out_shape=[
            pltpu.VMEM((rows, columns), bf16),
            pltpu.VMEM((rows, columns), bf16),
            pltpu.VMEM((rows, LANES), f32),
            pltpu.VMEM((1, columns), f32),
            pltpu.VMEM((1, rows), f32),
            pltpu.VMEM((1, width), f32),
        ],
        in_specs=[pl.BlockSpec(memory_space=pltpu.SMEM)] * 2 + [hbm] * 4,
        out_specs=[vmem] * 6,
        scratch_shapes=[
            pltpu.VMEM((rows, LANES), f32),
            pltpu.VMEM((n, 1, width), f32),
            pltpu.VMEM((n - 1, 1, width), f32),
            pltpu.VMEM((1, width + 2 * LANES), f32),
            pltpu.VMEM((n - 1, 1, width + 2 * LANES), f32),
            pltpu.VMEM((1, LANES), f32),
            pltpu.VMEM((experts - 1, 1, LANES), f32),
            pltpu.VMEM((1, rows), f32),
            pltpu.VMEM((1, width), f32),
            dma((2,)), dma((n,)), dma((n,)), dma((experts - 1,)), dma((experts - 1,)),
            dma((n - 1,)), dma((n - 1,)), dma((n - 1,)), dma((n - 1,)),
        ],
        compiler_params=pltpu.CompilerParams(
            collective_id=0, has_side_effects=True, vmem_limit_bytes=8 * 2**20
        ),
        name="statistics",
    )(
        step.reshape(1), prev_msq.reshape(1),
        *(
            pltpu.with_memory_space_constraint(x, pltpu.HBM)
            for x in (row_state, col_state, gradient.reshape(rows, columns), weight.reshape(rows, columns))
        )
    )
    block = block_width(columns)
    new_weight, new_row, new_col, msq = pl.pallas_call(
        functools.partial(update_kernel, block),
        out_shape=[
            jax.ShapeDtypeStruct((rows, columns), bf16),
            jax.ShapeDtypeStruct((1, rows), f32),
            jax.ShapeDtypeStruct((1, width), f32),
            jax.ShapeDtypeStruct((1, 1), f32),
        ],
        in_specs=[vmem] * 6,
        out_specs=[hbm, vmem, vmem, vmem],
        scratch_shapes=[pltpu.VMEM((2, rows, block), bf16), dma((2,))],
        compiler_params=pltpu.CompilerParams(vmem_limit_bytes=8 * 2**20),
        name="update",
    )(g, w, scale, factor, new_row, new_col)
    return (new_weight.reshape(1, rows, columns), new_row, new_col, msq)


def solution(mesh):
    split = P("expert", "rows")
    whole = P("expert", "rows", None)
    return jax.shard_map(
        shards,
        mesh=mesh,
        in_specs=(P(), whole, whole, split, split, split),
        out_specs=(whole, split, split, split),
        check_vma=False,
    )
```
